32 devices in a mesh: section: 16 (over z, x, core), dp: 2 (over y).
Axes of the slice: x: 2, y: 2, z: 4, core: 2. Of those that a mesh axis runs over, the one named last changes fastest.
Arguments:
- cotangent: bfloat16 [128, 8192], P('dp'), may hold values from -96 to 96
- lengths: int32 [4], P('dp'), may hold values from 1 to 32, as said below
- example_ids: int32 [128], P('dp'), may hold values from -1 to 3, as said below
- layer_inputs: bfloat16 [128, 32768], P('dp', 'section'), may hold values from -6 to 6
- preacts: bfloat16 [128, 32768], P('dp', 'section'), may hold values from -6 to 6
- weights: bfloat16 [32768, 8192], P('section', 'dp'), may hold values from -0.0625 to 0.0625
- query_left: bfloat16 [32768, 256], P('section'), may hold values from -0.0625 to 0.0625
- query_right: bfloat16 [32768, 256], P('section'), may hold values from -0.0625 to 0.0625
Outputs:
- input_grads: bfloat16 [128, 32768], P('dp', 'section')
- scores: float32 [4, 16], P('dp')
The draws below stay inside these ranges and needn't reach their ends.
Inputs may be any that keep to these rules, and one draw needn't show every extreme that they name: In each aligned block of 2 sequences one length is exactly 32; the lengths of a block sum to at most 64. `example_ids`: rows n * 64 to (n + 1) * 64 - 1 hold sequences n * 2 to (n + 1) * 2 - 1 in order from the block's first row, each on as many consecutive rows as its length; the block's remaining rows hold -1.
All inputs are finite; a program needn't handle non-finite values.
Results may differ from the reference program's by a relative error of at most 0.0066.
Values may be sent and summed in bfloat16 or wider, within the bound.
No kernel may reach another device: no remote copies, remote signals or barrier semaphores. Data moves between devices by JAX's collectives and lax.ppermute only.
A program may use at most 64 MiB of HBM per device.

```python
import jax
import jax.numpy as jnp
from jax import lax

D = 8192
LAYERS = 4
QUERIES = 16
RANK = 16
TOK_DEV = 64
SEQ_DEV = 2
QK = 256
MAXLEN = 32
SEQS = 4
TOKENS = 128


def packing(key):
    groups = SEQS // SEQ_DEV
    divisor_bits = jax.random.bits(jax.random.fold_in(key, 4101), (groups, SEQ_DEV), jnp.uint32)
    chosen_bits = jax.random.bits(jax.random.fold_in(key, 4207), (groups, 1), jnp.uint32)
    divisor = (divisor_bits % 6).astype(jnp.int32) + 1
    chosen = (chosen_bits % SEQ_DEV).astype(jnp.int32)
    spans = jnp.maximum(MAXLEN // divisor, 1)
    slot_ids = jnp.arange(SEQ_DEV, dtype=jnp.int32)[None, :]
    spans = jnp.where(slot_ids == chosen, MAXLEN, spans).astype(jnp.int32)
    run_ends = jnp.cumsum(spans, axis=1)
    row_ids = jnp.arange(TOK_DEV, dtype=jnp.int32)
    before = jnp.sum((row_ids[None, :, None] >= run_ends[:, None, :]).astype(jnp.int32), axis=2)
    live_total = run_ends[:, -1:]
    owners = jnp.arange(groups, dtype=jnp.int32)[:, None] * SEQ_DEV + before
    token_ids = jnp.where(row_ids[None, :] < live_total, owners, -1)
    return (spans.reshape(SEQS).astype(jnp.int32), token_ids.reshape(TOKENS).astype(jnp.int32))


def draw_lengths(key, part):
    return packing(key)[0]


def draw_example_ids(key, part):
    return packing(key)[1]


def steps_of(own_key, dims, shards, smallest, high):
    gain, own = 1.0, jax.random.fold_in(own_key, 6)
    for position, parts in shards:
        steps = jnp.exp(jax.random.uniform(jax.random.fold_in(own, position), (parts,), jnp.float32, smallest / len(shards), high / len(shards)))
        gain = gain * jnp.repeat(steps, dims[position] // parts).reshape([-1 if axis == position else 1 for axis in range(len(dims))])
    return gain


def scatter_about(own_key, shape, deviation, limit, split=(), kind=jnp.bfloat16):
    array = jax.random.normal(own_key, shape, jnp.float32) * deviation
    if len(split) > 0:
        array = steps_of(own_key, shape, split, -0.22, 0.18) * array
    return jnp.clip(array, min=-limit, max=limit).astype(kind)


def setup_inputs(seed: int = 0) -> dict:
    streams_of = jax.random.split(jax.random.key(seed), 9)
    cotangent = scatter_about(streams_of[0], (TOKENS, D), (MAXLEN // 2), 96.0, ((0, 2),))
    lengths = draw_lengths(jax.random.fold_in(streams_of[8], 71), 0)
    example_ids = draw_example_ids(jax.random.fold_in(streams_of[8], 71), 0)
    layer_inputs = scatter_about(streams_of[3], (TOKENS, LAYERS * D), 1.0, 6.0, ((0, 2), (1, 16)))
    preacts = scatter_about(streams_of[4], (TOKENS, LAYERS * D), 1.0, 6.0, ((0, 2), (1, 16)))
    weights = scatter_about(streams_of[5], (LAYERS * D, D), D ** -0.5, 0.0625, ((0, 16), (1, 2)))
    query_left = scatter_about(streams_of[6], (LAYERS * D, QK), D ** -0.5, 0.0625, ((0, 16),))
    query_right = scatter_about(streams_of[7], (LAYERS * D, QK), D ** -0.5, 0.0625, ((0, 16),))
    return dict(cotangent=cotangent, lengths=lengths, example_ids=example_ids, layer_inputs=layer_inputs, preacts=preacts, weights=weights, query_left=query_left, query_right=query_right)


def silu_slope(preact):
    sigmoid_value = jax.nn.sigmoid(preact)
    return sigmoid_value * (1.0 + preact * (1.0 - sigmoid_value))


def reference(cotangent, lengths, example_ids, layer_inputs, preacts, weights, query_left, query_right):
    seq_slots = jnp.arange(SEQS, dtype=jnp.int32)
    member = (example_ids[:, None] == seq_slots[None, :]).astype(jnp.float32)
    token_len = jnp.dot(member, lengths.astype(jnp.float32), precision=lax.Precision.HIGHEST)
    token_scale = jnp.where(example_ids >= 0, 1.0 / jnp.maximum(token_len, 1.0), 0.0)
    grad_out = (cotangent.astype(jnp.float32) * token_scale[:, None]).astype(jnp.bfloat16)
    scores = jnp.zeros((SEQS, QUERIES), jnp.float32)
    layer_grads = []
    for layer_index in reversed(range(LAYERS)):
        first_col = layer_index * D
        preact = preacts[:, first_col:first_col + D].astype(jnp.float32)
        gate_grad = (silu_slope(preact) * grad_out.astype(jnp.float32)).astype(jnp.bfloat16)
        layer_weight = weights[first_col:first_col + D, :]
        backward = lax.dot_general(gate_grad, layer_weight, (((1,), (1,)), ((), ())), preferred_element_type=jnp.float32)
        in_grad = (grad_out.astype(jnp.float32) + backward).astype(jnp.bfloat16)
        left_part = jnp.dot(layer_inputs[:, first_col:first_col + D], query_left[first_col:first_col + D], preferred_element_type=jnp.float32)
        right_part = jnp.dot(gate_grad, query_right[first_col:first_col + D], preferred_element_type=jnp.float32)
        per_token = jnp.sum((left_part * right_part).reshape(TOKENS, QUERIES, RANK), axis=2)
        scores = scores + jnp.dot(member.T, per_token, precision=lax.Precision.HIGHEST)
        layer_grads.insert(0, in_grad)
        grad_out = in_grad
    return jnp.concatenate(layer_grads, axis=1), scores
```

```python
import jax
import jax.numpy as jnp
from jax import lax
from jax.experimental import pallas as pl
from jax.experimental.pallas import tpu as pltpu
from jax.sharding import PartitionSpec as P

LAYERS = 4
QUERIES = 16
RANK = 16
CHUNKS = 2
AXES = ("section", "dp")


def spot():
    groups = lax.axis_size("dp")
    blocks = lax.axis_size("section") // LAYERS
    cores = blocks // groups
    position = lax.axis_index("section")
    block = lax.rem(position, blocks)
    return (
        lax.div(position, blocks),
        block,
        lax.div(block, cores),
        lax.rem(block, cores),
        lax.axis_index("dp"),
    )


def silu_slope(preact):
    sigmoid_value = jax.nn.sigmoid(preact)
    return sigmoid_value * (1.0 + preact * (1.0 - sigmoid_value))


VMEM = pl.BlockSpec(memory_space=pltpu.VMEM)
HBM = pl.BlockSpec(memory_space=pltpu.HBM)
ANY = pl.BlockSpec(memory_space=pl.ANY)


def small():
    return pltpu.CompilerParams(vmem_limit_bytes=12 * 2**20)


def load(weights, chunk, cores, after=(), pieces=8):
    rows = weights.shape[0] // pieces
    part = weights.shape[1] // (cores * CHUNKS)

    def body(weight_ref, *refs):
        out_ref, sems = refs[-2:]
        copies = []
        for k in range(cores):
            for i in range(pieces):
                span = pl.ds(i * rows, rows)
                source = weight_ref.at[span, pl.ds((k * CHUNKS + chunk) * part, part)]
                goal = out_ref.at[span, pl.ds(k * part, part)]
                copies.append(pltpu.make_async_copy(source, goal, sems.at[k, i]))
        for copy in copies:
            copy.start()
        for copy in copies:
            copy.wait()

    return pl.pallas_call(
        body,
        in_specs=[HBM] + [ANY] * len(after),
        out_specs=VMEM,
        out_shape=pltpu.VMEM((weights.shape[0], cores * part), weights.dtype),
        scratch_shapes=[pltpu.SemaphoreType.DMA((cores, pieces))],
        compiler_params=small(),
    )(pltpu.with_memory_space_constraint(weights, pltpu.HBM), *after)


def begin(lengths, ids, preacts, cotangent):
    tokens, width = preacts.shape
    part = width // CHUNKS
    seqs = lengths.shape[0]

    def body(length_ref, id_ref, preact_ref, cotangent_ref, *refs):
        layer, block, _, _, group = spot()
        top_ref = refs[0]
        buffer, sem, preact_buffer, preact_sem = refs[-8:-4]
        id_buffer, id_sem, length_buffer, length_sem = refs[-4:]
        column = pl.multiple_of(block * width, width)
        copy = pltpu.make_async_copy(cotangent_ref.at[:, pl.ds(column, width)], buffer, sem)
        copies = [
            copy,
            pltpu.make_async_copy(preact_ref, preact_buffer, preact_sem),
            pltpu.make_async_copy(id_ref, id_buffer, id_sem),
            pltpu.make_async_copy(length_ref, length_buffer, length_sem),
        ]
        for one in copies:
            one.start()
        for one in copies:
            one.wait()
        preact = preact_buffer[...]
        slope = silu_slope(preact.astype(jnp.float32))
        scale = jnp.zeros((1, tokens), jnp.float32)
        for n in range(seqs):
            count = jnp.full((1, tokens), length_buffer[n], jnp.int32).astype(jnp.float32)
            mine = id_buffer[...] == group * seqs + n
            scale = jnp.where(mine, 1.0 / jnp.maximum(count, 1.0), scale)
        row = lax.broadcasted_iota(jnp.int32, (tokens, tokens), 0)
        lane = lax.broadcasted_iota(jnp.int32, (tokens, tokens), 1)
        scale = jnp.sum(jnp.where(row == lane, scale, 0.0), axis=1, keepdims=True)
        top = (buffer[...].astype(jnp.float32) * scale).astype(jnp.bfloat16)
        top_ref[...] = top
        gate = (slope * top.astype(jnp.float32)).astype(jnp.bfloat16)
        value = jnp.where(layer == LAYERS - 1, gate, preact)
        for n in range(CHUNKS):
            refs[1 + n][...] = value[:, n * part : (n + 1) * part]

    outs = pl.pallas_call(
        body,
        in_specs=[HBM, HBM, HBM, HBM],
        out_specs=[VMEM] * (1 + CHUNKS),
        out_shape=[jax.ShapeDtypeStruct((tokens, width), jnp.bfloat16)]
        + [jax.ShapeDtypeStruct((tokens, part), jnp.bfloat16)] * CHUNKS,
        scratch_shapes=[
            pltpu.VMEM((tokens, width), jnp.bfloat16),
            pltpu.SemaphoreType.DMA(()),
            pltpu.VMEM((tokens, width), jnp.bfloat16),
            pltpu.SemaphoreType.DMA(()),
            pltpu.VMEM((1, tokens), jnp.int32),
            pltpu.SemaphoreType.DMA(()),
            pltpu.SMEM((seqs,), jnp.int32),
            pltpu.SemaphoreType.DMA(()),
        ],
        compiler_params=small(),
    )(
        *[
            pltpu.with_memory_space_constraint(value, pltpu.HBM)
            for value in (lengths, ids, preacts, cotangent)
        ],
    )
    return outs[0], outs[1:]


def product_body(
    lhs_ref, weight_ref, *refs, tick, distance, first_row, row_count, groups, cores, has_acc, splits
):
    outs = refs[1:] if has_acc else refs
    width = lhs_ref.shape[1]
    layer, _, place, core, group = spot()
    column = pl.multiple_of(lax.rem(core + distance, cores) * width, width)
    tile = min(512, row_count)

    @pl.when(layer == LAYERS - 1 - tick)
    def _():
        lhs = lhs_ref[...]
        for start in range(0, row_count, tile):
            weight = weight_ref[pl.ds(first_row + start, tile), pl.ds(column, width)]
            value = lax.dot_general(
                weight, lhs, (((1,), (1,)), ((), ())), preferred_element_type=jnp.float32
            )
            if has_acc:
                value = value + refs[0][pl.ds(first_row + start, tile), :]
            if splits:
                outs[-1][:, pl.ds(start, tile)] = value.T
            else:
                outs[0][pl.ds(start, tile), :] = value
        if splits:
            count = lhs.shape[0] // groups
            for slot in range(groups):
                first = pl.multiple_of(lax.rem(group + slot - place + groups, groups) * count, count)
                outs[slot][...] = outs[-1][pl.ds(first, count), :].astype(outs[slot].dtype)


def product(
    lhs, weights, acc, tick, distance, first_row, row_count, groups, cores, splits, after=()
):
    tokens = lhs.shape[0]
    width = lhs.shape[1]
    specs = [VMEM, VMEM]
    operands = [lhs, pltpu.with_memory_space_constraint(weights, pltpu.VMEM)]
    if acc is not None:
        specs.append(VMEM)
        operands.append(pltpu.with_memory_space_constraint(acc, pltpu.VMEM))
    used = len(specs)
    specs += [ANY] * len(after)
    operands += after
    scratch = []
    if splits:
        rows = tokens // groups
        kinds = [jnp.float32] + [jnp.bfloat16] * (groups - 1)
        out_shape = [jax.ShapeDtypeStruct((rows, row_count), kind) for kind in kinds]
        out_specs = [VMEM for _ in kinds]
        scratch = [pltpu.VMEM((tokens, row_count), jnp.float32)]
    else:
        out_shape = pltpu.VMEM((row_count, tokens), jnp.float32)
        out_specs = VMEM

    def body(*refs):
        product_body(
            *refs[:used],
            *refs[used + len(after) :],
            tick=tick,
            distance=distance,
            first_row=first_row,
            row_count=row_count,
            groups=groups,
            cores=cores,
            has_acc=acc is not None,
            splits=splits,
        )

    return pl.pallas_call(
        body,
        in_specs=specs,
        out_specs=out_specs,
        scratch_shapes=scratch,
        out_shape=out_shape,
        compiler_params=small(),
        cost_estimate=pl.CostEstimate(
            flops=2 * tokens * width * row_count,
            bytes_accessed=2 * width * row_count,
            transcendentals=0,
        ),
    )(*operands)


def join(pieces, after):
    rows, width = pieces[0].shape

    def body(*refs):
        for n in range(len(pieces)):
            refs[-1][pl.ds(n * rows, rows), :] = refs[n][...]

    return pl.pallas_call(
        body,
        in_specs=[VMEM] * len(pieces) + [ANY] * len(after),
        out_specs=VMEM,
        out_shape=jax.ShapeDtypeStruct((rows * len(pieces), width), pieces[0].dtype),
        compiler_params=small(),
    )(*pieces, *after)


def combine(kept, arrived, residual, column, before):
    rows, width = kept.shape
    parts = len(arrived)

    def body(*refs):
        total = refs[0][...] + refs[1 + parts][:, pl.ds(column, width)].astype(jnp.float32)
        for ref in refs[1 : 1 + parts]:
            total = total + ref[...].astype(jnp.float32)
        value = total.astype(jnp.bfloat16)
        if before:
            outs = refs[2 + parts + len(before) :]
            for n in range(len(before)):
                outs[1][:, pl.ds(n * width, width)] = refs[2 + parts + n][...]
            outs[1][:, pl.ds(column, width)] = value
        else:
            outs = refs[2 + parts :]
        outs[0][...] = value

    out_shape = [jax.ShapeDtypeStruct((rows, width), jnp.bfloat16)]
    if before:
        out_shape.append(jax.ShapeDtypeStruct(residual.shape, jnp.bfloat16))
    operands = [kept, *arrived, residual, *before]
    return pl.pallas_call(
        body,
        in_specs=[VMEM] * len(operands),
        out_specs=[VMEM] * len(out_shape),
        out_shape=out_shape,
        compiler_params=small(),
    )(*operands)


def finish(parts, arrived, residual, earlier):
    rows = residual.shape[0]
    width = parts[0].shape[1]
    count = len(parts)
    per_part = len(arrived[0])

    def body(*refs):
        layer = spot()[0]
        out_ref = refs[-1]
        residual_ref = refs[count * (1 + per_part)]
        earlier_refs = refs[count * (1 + per_part) + 1 : -1]
        for n in range(count):
            span = pl.ds(n * width, width)
            total = refs[n][...] + residual_ref[:, span].astype(jnp.float32)
            for d in range(per_part):
                total = total + refs[count + n * per_part + d][...].astype(jnp.float32)
            value = total.astype(jnp.bfloat16)
            for tick, ref in enumerate(earlier_refs):
                value = jnp.where(layer == LAYERS - 1 - tick, ref[:, span], value)
            out_ref[:, span] = value

    operands = [*parts]
    for group in arrived:
        operands += group
    operands += [residual, *earlier]
    return pl.pallas_call(
        body,
        in_specs=[VMEM] * len(operands),
        out_specs=VMEM,
        out_shape=jax.ShapeDtypeStruct((rows, width * count), jnp.bfloat16),
        compiler_params=small(),
    )(*operands)


def left_side(values, factors):
    def body(value_ref, factor_ref, out_ref):
        out_ref[...] = jnp.dot(
            value_ref[...], factor_ref[...], preferred_element_type=jnp.float32
        )

    return pl.pallas_call(
        body,
        in_specs=[VMEM, VMEM],
        out_specs=VMEM,
        out_shape=jax.ShapeDtypeStruct((values.shape[0], factors.shape[1]), jnp.float32),
        compiler_params=small(),
    )(values, factors)


def score_terms(ids, preacts, candidates, factors, left, seqs):
    def body(id_ref, preact_ref, *refs):
        layer, _, _, _, group = spot()
        factor_ref, left_ref, out_ref = refs[-3:]
        value = refs[0][...]
        for tick, ref in enumerate(refs[1:-3]):
            value = jnp.where(layer == LAYERS - 2 - tick, ref[...], value)
        slope = silu_slope(preact_ref[...].astype(jnp.float32))
        gate = (slope * value.astype(jnp.float32)).astype(jnp.bfloat16)
        right = jnp.dot(gate, factor_ref[...], preferred_element_type=jnp.float32)
        terms = left_ref[...] * right
        rank = lax.broadcasted_iota(jnp.int32, (terms.shape[1], QUERIES), 0) // RANK
        query = lax.broadcasted_iota(jnp.int32, (terms.shape[1], QUERIES), 1)
        pick = (rank == query).astype(jnp.float32)
        tokens = terms.shape[0]
        slot = group * seqs + lax.broadcasted_iota(jnp.int32, (seqs, tokens), 0)
        member = (id_ref[...] == slot).astype(jnp.float32)
        total = jnp.dot(
            member, terms, preferred_element_type=jnp.float32, precision=lax.Precision.HIGHEST
        )
        out_ref[...] = jnp.dot(
            total, pick, preferred_element_type=jnp.float32, precision=lax.Precision.HIGHEST
        )

    operands = [ids, preacts, *candidates, factors, left]
    return pl.pallas_call(
        body,
        in_specs=[VMEM] * len(operands),
        out_specs=VMEM,
        out_shape=jax.ShapeDtypeStruct((seqs, QUERIES), jnp.float32),
        compiler_params=small(),
    )(*operands)


def per_device(
    cotangent, lengths, example_ids, layer_inputs, preacts, weights, query_left, query_right
):
    blocks = lax.axis_size("section") // LAYERS
    groups = lax.axis_size("dp")
    cores = blocks // groups
    tokens = cotangent.shape[0]
    width = layer_inputs.shape[1]
    part = width // CHUNKS
    seqs = lengths.shape[0]

    def device(s, h, k, y):
        return ((s * blocks) + h * cores + k) * groups + y

    everyone = [
        (s, h, k, y)
        for s in range(LAYERS)
        for h in range(groups)
        for k in range(cores)
        for y in range(groups)
    ]

    def send(value, target):
        pairs = []
        for spot in everyone:
            goal = target(*spot)
            if goal[0] >= 0:
                pairs.append((device(*spot), device(*goal)))
        return lax.ppermute(value, AXES, pairs)

    def turned(value):
        return send(value, lambda s, h, k, y: (s, y, k, h))

    def lowered(value, tick, turn):
        def target(s, h, k, y):
            if s != LAYERS - 1 - tick:
                return (-1, 0, 0, 0)
            return (s - 1, y, k, h) if turn else (s - 1, h, k, y)

        return send(value, target)

    def from_places(value):
        return [
            send(value, lambda s, h, k, y: (s, (h - d) % groups, k, y))
            for d in range(1, groups)
        ]

    def from_cores(value):
        return [
            send(value, lambda s, h, k, y: (s, h, (k - d) % cores, y)) for d in range(1, cores)
        ]

    def sum_over(value, axis, count):
        step = 1
        while step < count:
            if axis == "core":
                value = value + send(value, lambda s, h, k, y: (s, h, k ^ step, y))
            elif axis == "place":
                value = value + send(value, lambda s, h, k, y: (s, h ^ step, k, y))
            else:
                value = value + send(value, lambda s, h, k, y: (s ^ step, h, k, y))
            step *= 2
        return value

    id_row = example_ids.reshape(1, tokens)
    top_grad, payload = begin(lengths, id_row, preacts, cotangent)

    turned_payload = [turned(payload[o]) for o in range(CHUNKS)]
    slope_turned = [silu_slope(value.astype(jnp.float32)) for value in turned_payload]
    held = [load(weights, 0, cores, [turned_payload[0]])]
    gates = [turned_payload[0]]
    for o in range(1, CHUNKS):
        gates.append(join([turned_payload[o]], [held[o - 1]]))
        held.append(load(weights, o, cores, [gates[o]]))
    left_sum = left_side(layer_inputs, query_left)
    residual = top_grad
    candidates = [top_grad]
    sums = []
    for tick in range(LAYERS):
        last = tick == LAYERS - 1
        acc = None
        parts = []
        mine_sent = [from_places(gates[o]) for o in range(CHUNKS)]
        behind = []
        if tick == 1:
            left_sum = sum_over(left_sum, "core", cores)
            behind = [left_sum]
        if tick == 2:
            left_sum = sum_over(left_sum, "place", groups)
            behind = [left_sum]
        if last:
            terms = score_terms(id_row, preacts, candidates, query_right, left_sum, seqs)
            terms = sum_over(terms, "core", cores)
            behind = [terms]
            terms = sum_over(terms, "place", groups)
        for o in range(CHUNKS):
            mine = join([gates[o]] + mine_sent[o], [] if acc is None else [acc])
            pieces = [mine] + from_cores(mine)
            for k in range(cores):
                if o == CHUNKS - 1 and k == cores - 1:
                    for n in range(CHUNKS):
                        parts.append(
                            product(
                                pieces[k], held[o], acc, tick, k, n * part, part, groups, cores,
                                True, behind + [p[0] for p in parts[:n]],
                            )
                        )
                else:
                    acc = product(
                        pieces[k], held[o], acc, tick, k, 0, width, groups, cores, False,
                        held[1:] if tick + o + k == 0 else [],
                    )
        arrived = []
        for n in range(CHUNKS):
            arrived.append(
                [
                    send(parts[n][d], lambda s, h, k, y: (s, h, k, (y + d) % groups))
                    for d in range(1, groups)
                ]
            )
        kept = [piece[0] for piece in parts]
        if last:
            break
        in_parts = []
        for n in range(CHUNKS):
            outs = combine(
                kept[n], arrived[n], residual, n * part, in_parts if n == CHUNKS - 1 else []
            )
            in_parts.append(outs[0])
        in_grad = outs[1]
        sums.append(in_grad)
        gates = []
        for n in range(CHUNKS):
            came = lowered(in_parts[n], tick, True)
            gates.append((slope_turned[n] * came.astype(jnp.float32)).astype(jnp.bfloat16))
        residual = lowered(in_grad, tick, False)
        candidates.append(residual)

    result = finish(kept, arrived, residual, sums)
    scores = sum_over(terms, "layer", LAYERS)
    return (result, scores)


def solution(mesh):
    placed = (
        P("dp", None),
        P("dp"),
        P("dp"),
        P("dp", "section"),
        P("dp", "section"),
        P("section", "dp"),
        P("section", None),
        P("section", None),
    )
    return jax.shard_map(
        per_device,
        mesh=mesh,
        in_specs=placed,
        out_specs=(P("dp", "section"), P("dp", None)),
        check_vma=False,
    )
```

```python
import jax
import jax.numpy as jnp
from jax import lax
from jax.experimental import pallas as pl
from jax.experimental.pallas import tpu as pltpu
from jax.sharding import PartitionSpec as P

LAYERS = 4
QUERIES = 16
RANK = 16
CHUNKS = 2
AXES = ("section", "dp")


def spot():
    groups = lax.axis_size("dp")
    blocks = lax.axis_size("section") // LAYERS
    cores = blocks // groups
    position = lax.axis_index("section")
    block = lax.rem(position, blocks)
    return (
        lax.div(position, blocks),
        block,
        lax.div(block, cores),
        lax.rem(block, cores),
        lax.axis_index("dp"),
    )


def silu_slope(preact):
    sigmoid_value = jax.nn.sigmoid(preact)
    return sigmoid_value * (1.0 + preact * (1.0 - sigmoid_value))


VMEM = pl.BlockSpec(memory_space=pltpu.VMEM)
HBM = pl.BlockSpec(memory_space=pltpu.HBM)
ANY = pl.BlockSpec(memory_space=pl.ANY)


def small():
    return pltpu.CompilerParams(vmem_limit_bytes=12 * 2**20)


def load(weights, chunk, cores, after=(), pieces=8):
    rows = weights.shape[0] // pieces
    part = weights.shape[1] // (cores * CHUNKS)

    def body(weight_ref, *refs):
        out_ref, sems = refs[-2:]
        copies = []
        for k in range(cores):
            for i in range(pieces):
                span = pl.ds(i * rows, rows)
                source = weight_ref.at[span, pl.ds((k * CHUNKS + chunk) * part, part)]
                goal = out_ref.at[span, pl.ds(k * part, part)]
                copies.append(pltpu.make_async_copy(source, goal, sems.at[k, i]))
        for copy in copies:
            copy.start()
        for copy in copies:
            copy.wait()

    return pl.pallas_call(
        body,
        in_specs=[HBM] + [ANY] * len(after),
        out_specs=VMEM,
        out_shape=pltpu.VMEM((weights.shape[0], cores * part), weights.dtype),
        scratch_shapes=[pltpu.SemaphoreType.DMA((cores, pieces))],
        compiler_params=small(),
    )(pltpu.with_memory_space_constraint(weights, pltpu.HBM), *after)


def begin(lengths, ids, preacts, cotangent):
    tokens, width = preacts.shape
    seqs = lengths.shape[0]

    def body(length_ref, id_ref, preact_ref, cotangent_ref, *refs):
        layer, block, _, _, group = spot()
        top_ref = refs[0]
        buffer, sem, preact_buffer, preact_sem = refs[-8:-4]
        id_buffer, id_sem, length_buffer, length_sem = refs[-4:]
        column = pl.multiple_of(block * width, width)
        copy = pltpu.make_async_copy(cotangent_ref.at[:, pl.ds(column, width)], buffer, sem)
        copies = [
            copy,
            pltpu.make_async_copy(preact_ref, preact_buffer, preact_sem),
            pltpu.make_async_copy(id_ref, id_buffer, id_sem),
            pltpu.make_async_copy(length_ref, length_buffer, length_sem),
        ]
        for one in copies:
            one.start()
        for one in copies:
            one.wait()
        preact = preact_buffer[...]
        slope = silu_slope(preact.astype(jnp.float32))
        scale = jnp.zeros((1, tokens), jnp.float32)
        for n in range(seqs):
            count = jnp.full((1, tokens), length_buffer[n], jnp.int32).astype(jnp.float32)
            mine = id_buffer[...] == group * seqs + n
            scale = jnp.where(mine, 1.0 / jnp.maximum(count, 1.0), scale)
        row = lax.broadcasted_iota(jnp.int32, (tokens, tokens), 0)
        lane = lax.broadcasted_iota(jnp.int32, (tokens, tokens), 1)
        scale = jnp.sum(jnp.where(row == lane, scale, 0.0), axis=1, keepdims=True)
        top = (buffer[...].astype(jnp.float32) * scale).astype(jnp.bfloat16)
        top_ref[...] = top
        gate = (slope * top.astype(jnp.float32)).astype(jnp.bfloat16)
        refs[1][...] = jnp.where(layer == LAYERS - 1, gate, preact)

    return pl.pallas_call(
        body,
        in_specs=[HBM, HBM, HBM, HBM],
        out_specs=[VMEM] * 2,
        out_shape=[jax.ShapeDtypeStruct((tokens, width), jnp.bfloat16)] * 2,
        scratch_shapes=[
            pltpu.VMEM((tokens, width), jnp.bfloat16),
            pltpu.SemaphoreType.DMA(()),
            pltpu.VMEM((tokens, width), jnp.bfloat16),
            pltpu.SemaphoreType.DMA(()),
            pltpu.VMEM((1, tokens), jnp.int32),
            pltpu.SemaphoreType.DMA(()),
            pltpu.SMEM((seqs,), jnp.int32),
            pltpu.SemaphoreType.DMA(()),
        ],
        compiler_params=small(),
    )(
        *[
            pltpu.with_memory_space_constraint(value, pltpu.HBM)
            for value in (lengths, ids, preacts, cotangent)
        ],
    )


def product_body(
    lhs_ref, weight_ref, *refs, tick, distance, first_row, row_count, groups, cores, has_acc, splits
):
    outs = refs[1:] if has_acc else refs
    width = lhs_ref.shape[1]
    layer, _, place, core, group = spot()
    column = pl.multiple_of(lax.rem(core + distance, cores) * width, width)
    tile = min(512, row_count)

    @pl.when(layer == LAYERS - 1 - tick)
    def _():
        lhs = lhs_ref[...]
        for start in range(0, row_count, tile):
            weight = weight_ref[pl.ds(first_row + start, tile), pl.ds(column, width)]
            value = lax.dot_general(
                weight, lhs, (((1,), (1,)), ((), ())), preferred_element_type=jnp.float32
            )
            if has_acc:
                value = value + refs[0][pl.ds(first_row + start, tile), :]
            if splits:
                outs[-1][:, pl.ds(start, tile)] = value.T
            else:
                outs[0][pl.ds(start, tile), :] = value
        if splits:
            count = lhs.shape[0] // groups
            for slot in range(groups):
                first = pl.multiple_of(lax.rem(group + slot - place + groups, groups) * count, count)
                outs[slot][...] = outs[-1][pl.ds(first, count), :].astype(outs[slot].dtype)


def product(
    lhs, weights, acc, tick, distance, first_row, row_count, groups, cores, splits, after=()
):
    tokens = lhs.shape[0]
    width = lhs.shape[1]
    specs = [VMEM, VMEM]
    operands = [lhs, pltpu.with_memory_space_constraint(weights, pltpu.VMEM)]
    if acc is not None:
        specs.append(VMEM)
        operands.append(pltpu.with_memory_space_constraint(acc, pltpu.VMEM))
    used = len(specs)
    specs += [ANY] * len(after)
    operands += after
    scratch = []
    if splits:
        rows = tokens // groups
        kinds = [jnp.float32] + [jnp.bfloat16] * (groups - 1)
        out_shape = [jax.ShapeDtypeStruct((rows, row_count), kind) for kind in kinds]
        out_specs = [VMEM for _ in kinds]
        scratch = [pltpu.VMEM((tokens, row_count), jnp.float32)]
    else:
        out_shape = pltpu.VMEM((row_count, tokens), jnp.float32)
        out_specs = VMEM

    def body(*refs):
        product_body(
            *refs[:used],
            *refs[used + len(after) :],
            tick=tick,
            distance=distance,
            first_row=first_row,
            row_count=row_count,
            groups=groups,
            cores=cores,
            has_acc=acc is not None,
            splits=splits,
        )

    return pl.pallas_call(
        body,
        in_specs=specs,
        out_specs=out_specs,
        scratch_shapes=scratch,
        out_shape=out_shape,
        compiler_params=small(),
        cost_estimate=pl.CostEstimate(
            flops=2 * tokens * width * row_count,
            bytes_accessed=2 * width * row_count,
            transcendentals=0,
        ),
    )(*operands)


def join(pieces, after):
    rows, width = pieces[0].shape

    def body(*refs):
        for n in range(len(pieces)):
            refs[-1][pl.ds(n * rows, rows), :] = refs[n][...]

    return pl.pallas_call(
        body,
        in_specs=[VMEM] * len(pieces) + [ANY] * len(after),
        out_specs=VMEM,
        out_shape=jax.ShapeDtypeStruct((rows * len(pieces), width), pieces[0].dtype),
        compiler_params=small(),
    )(*pieces, *after)


def gate(grads, preacts, column):
    rows, width = grads.shape

    def body(grad_ref, preact_ref, out_ref):
        slope = silu_slope(preact_ref[:, pl.ds(column, width)].astype(jnp.float32))
        out_ref[...] = (slope * grad_ref[...].astype(jnp.float32)).astype(jnp.bfloat16)

    return pl.pallas_call(
        body,
        in_specs=[VMEM, VMEM],
        out_specs=VMEM,
        out_shape=jax.ShapeDtypeStruct((rows, width), jnp.bfloat16),
        compiler_params=small(),
    )(grads, preacts)


def combine(kept, arrived, residual, column, before):
    rows, width = kept.shape
    parts = len(arrived)

    def body(*refs):
        total = refs[0][...] + refs[1 + parts][:, pl.ds(column, width)].astype(jnp.float32)
        for ref in refs[1 : 1 + parts]:
            total = total + ref[...].astype(jnp.float32)
        value = total.astype(jnp.bfloat16)
        if before:
            outs = refs[2 + parts + len(before) :]
            for n in range(len(before)):
                outs[1][:, pl.ds(n * width, width)] = refs[2 + parts + n][...]
            outs[1][:, pl.ds(column, width)] = value
        else:
            outs = refs[2 + parts :]
        outs[0][...] = value

    out_shape = [jax.ShapeDtypeStruct((rows, width), jnp.bfloat16)]
    if before:
        out_shape.append(jax.ShapeDtypeStruct(residual.shape, jnp.bfloat16))
    operands = [kept, *arrived, residual, *before]
    return pl.pallas_call(
        body,
        in_specs=[VMEM] * len(operands),
        out_specs=[VMEM] * len(out_shape),
        out_shape=out_shape,
        compiler_params=small(),
    )(*operands)


def finish(parts, arrived, residual, earlier, terms):
    rows = residual.shape[0]
    width = parts[0].shape[1]
    count = len(parts)
    per_part = len(arrived[0])

    def body(*refs):
        layer = spot()[0]
        out_ref, score_ref = refs[-2:]
        term_refs = refs[-2 - len(terms) : -2]
        residual_ref = refs[count * (1 + per_part)]
        earlier_refs = refs[count * (1 + per_part) + 1 : -2 - len(terms)]
        for n in range(count):
            span = pl.ds(n * width, width)
            total = refs[n][...] + residual_ref[:, span].astype(jnp.float32)
            for d in range(per_part):
                total = total + refs[count + n * per_part + d][...].astype(jnp.float32)
            value = total.astype(jnp.bfloat16)
            for tick, ref in enumerate(earlier_refs):
                value = jnp.where(layer == LAYERS - 1 - tick, ref[:, span], value)
            out_ref[:, span] = value
        values = [ref[...] for ref in term_refs]
        while len(values) > 1:
            values = [values[n] + values[n + 1] for n in range(0, len(values), 2)]
        score_ref[...] = values[0]

    operands = [*parts]
    for group in arrived:
        operands += group
    operands += [residual, *earlier, *terms]
    return pl.pallas_call(
        body,
        in_specs=[VMEM] * len(operands),
        out_specs=[VMEM, VMEM],
        out_shape=[
            jax.ShapeDtypeStruct((rows, width * count), jnp.bfloat16),
            jax.ShapeDtypeStruct(terms[0].shape, terms[0].dtype),
        ],
        compiler_params=small(),
    )(*operands)


def left_side(values, factors):
    def body(value_ref, factor_ref, out_ref):
        out_ref[...] = jnp.dot(
            value_ref[...], factor_ref[...], preferred_element_type=jnp.float32
        )

    return pl.pallas_call(
        body,
        in_specs=[VMEM, VMEM],
        out_specs=VMEM,
        out_shape=jax.ShapeDtypeStruct((values.shape[0], factors.shape[1]), jnp.float32),
        compiler_params=small(),
    )(values, factors)


def score_terms(ids, preacts, candidates, factors, left, seqs):
    def body(id_ref, preact_ref, *refs):
        layer, _, _, _, group = spot()
        factor_ref, left_ref, out_ref = refs[-3:]
        value = refs[0][...]
        for tick, ref in enumerate(refs[1:-3]):
            value = jnp.where(layer == LAYERS - 2 - tick, ref[...], value)
        slope = silu_slope(preact_ref[...].astype(jnp.float32))
        gate = (slope * value.astype(jnp.float32)).astype(jnp.bfloat16)
        right = jnp.dot(gate, factor_ref[...], preferred_element_type=jnp.float32)
        terms = left_ref[...] * right
        rank = lax.broadcasted_iota(jnp.int32, (terms.shape[1], QUERIES), 0) // RANK
        query = lax.broadcasted_iota(jnp.int32, (terms.shape[1], QUERIES), 1)
        pick = (rank == query).astype(jnp.float32)
        tokens = terms.shape[0]
        slot = group * seqs + lax.broadcasted_iota(jnp.int32, (seqs, tokens), 0)
        member = (id_ref[...] == slot).astype(jnp.float32)
        total = jnp.dot(
            member, terms, preferred_element_type=jnp.float32, precision=lax.Precision.HIGHEST
        )
        out_ref[...] = jnp.dot(
            total, pick, preferred_element_type=jnp.float32, precision=lax.Precision.HIGHEST
        )

    operands = [ids, preacts, *candidates, factors, left]
    return pl.pallas_call(
        body,
        in_specs=[VMEM] * len(operands),
        out_specs=VMEM,
        out_shape=jax.ShapeDtypeStruct((seqs, QUERIES), jnp.float32),
        compiler_params=small(),
    )(*operands)


def per_device(
    cotangent, lengths, example_ids, layer_inputs, preacts, weights, query_left, query_right
):
    blocks = lax.axis_size("section") // LAYERS
    groups = lax.axis_size("dp")
    cores = blocks // groups
    tokens = cotangent.shape[0]
    width = layer_inputs.shape[1]
    part = width // CHUNKS
    seqs = lengths.shape[0]

    def device(s, h, k, y):
        return ((s * blocks) + h * cores + k) * groups + y

    everyone = [
        (s, h, k, y)
        for s in range(LAYERS)
        for h in range(groups)
        for k in range(cores)
        for y in range(groups)
    ]

    def send(value, target):
        pairs = []
        for spot in everyone:
            goal = target(*spot)
            if goal[0] >= 0:
                pairs.append((device(*spot), device(*goal)))
        return lax.ppermute(value, AXES, pairs)

    def turned(value):
        return send(value, lambda s, h, k, y: (s, y, k, h))

    def lowered(value, tick, turn):
        def target(s, h, k, y):
            if s != LAYERS - 1 - tick:
                return (-1, 0, 0, 0)
            return (s - 1, y, k, h) if turn else (s - 1, h, k, y)

        return send(value, target)

    def from_places(value):
        return [
            send(value, lambda s, h, k, y: (s, (h - d) % groups, k, y))
            for d in range(1, groups)
        ]

    def from_cores(value):
        return [
            send(value, lambda s, h, k, y: (s, h, (k - d) % cores, y)) for d in range(1, cores)
        ]

    def sum_over(value, axis, count):
        step = 1
        while step < count:
            if axis == "core":
                value = value + send(value, lambda s, h, k, y: (s, h, k ^ step, y))
            elif axis == "place":
                value = value + send(value, lambda s, h, k, y: (s, h ^ step, k, y))
            else:
                value = value + send(value, lambda s, h, k, y: (s ^ step, h, k, y))
            step *= 2
        return value

    id_row = example_ids.reshape(1, tokens)
    top_grad, payload = begin(lengths, id_row, preacts, cotangent)

    turned_payload = turned(payload)
    gates = [turned_payload[:, o * part : (o + 1) * part] for o in range(CHUNKS)]
    held = [load(weights, o, cores) for o in range(CHUNKS)]
    left_sum = left_side(layer_inputs, query_left)
    residual = top_grad
    candidates = [top_grad]
    sums = []
    for tick in range(LAYERS):
        last = tick == LAYERS - 1
        acc = None
        parts = []
        mine_sent = [from_places(gates[o]) for o in range(CHUNKS)]
        behind = []
        if tick == 1:
            left_sum = sum_over(left_sum, "core", cores)
            behind = [left_sum]
        if tick == 2:
            left_sum = sum_over(left_sum, "place", groups)
            behind = [left_sum]
        if last:
            terms = score_terms(id_row, preacts, candidates, query_right, left_sum, seqs)
            terms = sum_over(terms, "core", cores)
            behind = [terms]
            terms = sum_over(terms, "place", groups)
        for o in range(CHUNKS):
            mine = join([gates[o]] + mine_sent[o], [] if acc is None else [acc])
            pieces = [mine] + from_cores(mine)
            for k in range(cores):
                if o == CHUNKS - 1 and k == cores - 1:
                    for n in range(CHUNKS):
                        parts.append(
                            product(
                                pieces[k], held[o], acc, tick, k, n * part, part, groups, cores,
                                True, behind + [p[0] for p in parts[:n]],
                            )
                        )
                else:
                    acc = product(pieces[k], held[o], acc, tick, k, 0, width, groups, cores, False)
        arrived = []
        for n in range(CHUNKS):
            arrived.append(
                [
                    send(parts[n][d], lambda s, h, k, y: (s, h, k, (y + d) % groups))
                    for d in range(1, groups)
                ]
            )
        kept = [piece[0] for piece in parts]
        if last:
            break
        in_parts = []
        for n in range(CHUNKS):
            outs = combine(
                kept[n], arrived[n], residual, n * part, in_parts if n == CHUNKS - 1 else []
            )
            in_parts.append(outs[0])
        in_grad = outs[1]
        sums.append(in_grad)
        gates = []
        for n in range(CHUNKS):
            came = lowered(in_parts[n], tick, True)
            gates.append(gate(came, turned_payload, n * part))
        residual = lowered(in_grad, tick, False)
        candidates.append(residual)

    everywhere = [terms]
    for d in range(1, LAYERS):
        everywhere.append(send(terms, lambda s, h, k, y: (s ^ d, h, k, y)))
    result, scores = finish(kept, arrived, residual, sums, everywhere)
    return (result, scores)


def solution(mesh):
    placed = (
        P("dp", None),
        P("dp"),
        P("dp"),
        P("dp", "section"),
        P("dp", "section"),
        P("section", "dp"),
        P("section", None),
        P("section", None),
    )
    return jax.shard_map(
        per_device,
        mesh=mesh,
        in_specs=placed,
        out_specs=(P("dp", "section"), P("dp", None)),
        check_vma=False,
    )
```

```python
import jax
import jax.numpy as jnp
from jax import lax
from jax.experimental import pallas as pl
from jax.experimental.pallas import tpu as pltpu
from jax.sharding import PartitionSpec as P

LAYERS = 4
QUERIES = 16
RANK = 16
CHUNKS = 2
AXES = ("section", "dp")


def spot():
    groups = lax.axis_size("dp")
    blocks = lax.axis_size("section") // LAYERS
    cores = blocks // groups
    position = lax.axis_index("section")
    block = lax.rem(position, blocks)
    return (
        lax.div(position, blocks),
        block,
        lax.div(block, cores),
        lax.rem(block, cores),
        lax.axis_index("dp"),
    )


def silu_slope(preact):
    sigmoid_value = jax.nn.sigmoid(preact)
    return sigmoid_value * (1.0 + preact * (1.0 - sigmoid_value))


VMEM = pl.BlockSpec(memory_space=pltpu.VMEM)
HBM = pl.BlockSpec(memory_space=pltpu.HBM)
ANY = pl.BlockSpec(memory_space=pl.ANY)


def small():
    return pltpu.CompilerParams(vmem_limit_bytes=12 * 2**20)


def load(weights, chunk, cores, after=(), pieces=8):
    rows = weights.shape[0] // pieces
    part = weights.shape[1] // (cores * CHUNKS)

    def body(weight_ref, *refs):
        out_ref, sems = refs[-2:]
        copies = []
        for k in range(cores):
            for i in range(pieces):
                span = pl.ds(i * rows, rows)
                source = weight_ref.at[span, pl.ds((k * CHUNKS + chunk) * part, part)]
                goal = out_ref.at[span, pl.ds(k * part, part)]
                copies.append(pltpu.make_async_copy(source, goal, sems.at[k, i]))
        for copy in copies:
            copy.start()
        for copy in copies:
            copy.wait()

    return pl.pallas_call(
        body,
        in_specs=[HBM] + [ANY] * len(after),
        out_specs=VMEM,
        out_shape=pltpu.VMEM((weights.shape[0], cores * part), weights.dtype),
        scratch_shapes=[pltpu.SemaphoreType.DMA((cores, pieces))],
        compiler_params=small(),
    )(pltpu.with_memory_space_constraint(weights, pltpu.HBM), *after)


def begin(lengths, ids, preacts, cotangent):
    tokens, width = preacts.shape
    seqs = lengths.shape[0]

    def body(length_ref, id_ref, preact_ref, cotangent_ref, *refs):
        layer, block, _, _, group = spot()
        top_ref = refs[0]
        buffer, sem, preact_buffer, preact_sem = refs[-8:-4]
        id_buffer, id_sem, length_buffer, length_sem = refs[-4:]
        column = pl.multiple_of(block * width, width)
        copy = pltpu.make_async_copy(cotangent_ref.at[:, pl.ds(column, width)], buffer, sem)
        copies = [
            copy,
            pltpu.make_async_copy(preact_ref, preact_buffer, preact_sem),
            pltpu.make_async_copy(id_ref, id_buffer, id_sem),
            pltpu.make_async_copy(length_ref, length_buffer, length_sem),
        ]
        for one in copies:
            one.start()
        for one in copies:
            one.wait()
        preact = preact_buffer[...]
        slope = silu_slope(preact.astype(jnp.float32))
        scale = jnp.zeros((1, tokens), jnp.float32)
        for n in range(seqs):
            count = jnp.full((1, tokens), length_buffer[n], jnp.int32).astype(jnp.float32)
            mine = id_buffer[...] == group * seqs + n
            scale = jnp.where(mine, 1.0 / jnp.maximum(count, 1.0), scale)
        row = lax.broadcasted_iota(jnp.int32, (tokens, tokens), 0)
        lane = lax.broadcasted_iota(jnp.int32, (tokens, tokens), 1)
        scale = jnp.sum(jnp.where(row == lane, scale, 0.0), axis=1, keepdims=True)
        top = (buffer[...].astype(jnp.float32) * scale).astype(jnp.bfloat16)
        top_ref[...] = top
        gate = (slope * top.astype(jnp.float32)).astype(jnp.bfloat16)
        refs[1][...] = jnp.where(layer == LAYERS - 1, gate, preact)

    return pl.pallas_call(
        body,
        in_specs=[HBM, HBM, HBM, HBM],
        out_specs=[VMEM] * 2,
        out_shape=[jax.ShapeDtypeStruct((tokens, width), jnp.bfloat16)] * 2,
        scratch_shapes=[
            pltpu.VMEM((tokens, width), jnp.bfloat16),
            pltpu.SemaphoreType.DMA(()),
            pltpu.VMEM((tokens, width), jnp.bfloat16),
            pltpu.SemaphoreType.DMA(()),
            pltpu.VMEM((1, tokens), jnp.int32),
            pltpu.SemaphoreType.DMA(()),
            pltpu.SMEM((seqs,), jnp.int32),
            pltpu.SemaphoreType.DMA(()),
        ],
        compiler_params=small(),
    )(
        *[
            pltpu.with_memory_space_constraint(value, pltpu.HBM)
            for value in (lengths, ids, preacts, cotangent)
        ],
    )


def product_body(
    lhs_ref, weight_ref, *refs, tick, distance, first_row, row_count, groups, cores, has_acc, splits
):
    outs = refs[1:] if has_acc else refs
    width = lhs_ref.shape[1]
    layer, _, place, core, group = spot()
    column = pl.multiple_of(lax.rem(core + distance, cores) * width, width)
    tile = min(512, row_count)

    @pl.when(layer == LAYERS - 1 - tick)
    def _():
        lhs = lhs_ref[...]
        for start in range(0, row_count, tile):
            weight = weight_ref[pl.ds(first_row + start, tile), pl.ds(column, width)]
            value = lax.dot_general(
                weight, lhs, (((1,), (1,)), ((), ())), preferred_element_type=jnp.float32
            )
            if has_acc:
                value = value + refs[0][pl.ds(first_row + start, tile), :]
            if splits:
                outs[-1][:, pl.ds(start, tile)] = value.T
            else:
                outs[0][pl.ds(start, tile), :] = value
        if splits:
            count = lhs.shape[0] // groups
            for slot in range(groups):
                first = pl.multiple_of(lax.rem(group + slot - place + groups, groups) * count, count)
                outs[slot][...] = outs[-1][pl.ds(first, count), :].astype(outs[slot].dtype)


def product(
    lhs, weights, acc, tick, distance, first_row, row_count, groups, cores, splits, after=()
):
    tokens = lhs.shape[0]
    width = lhs.shape[1]
    specs = [VMEM, VMEM]
    operands = [lhs, pltpu.with_memory_space_constraint(weights, pltpu.VMEM)]
    if acc is not None:
        specs.append(VMEM)
        operands.append(pltpu.with_memory_space_constraint(acc, pltpu.VMEM))
    used = len(specs)
    specs += [ANY] * len(after)
    operands += after
    scratch = []
    if splits:
        rows = tokens // groups
        kinds = [jnp.float32] + [jnp.bfloat16] * (groups - 1)
        out_shape = [jax.ShapeDtypeStruct((rows, row_count), kind) for kind in kinds]
        out_specs = [VMEM for _ in kinds]
        scratch = [pltpu.VMEM((tokens, row_count), jnp.float32)]
    else:
        out_shape = pltpu.VMEM((row_count, tokens), jnp.float32)
        out_specs = VMEM

    def body(*refs):
        product_body(
            *refs[:used],
            *refs[used + len(after) :],
            tick=tick,
            distance=distance,
            first_row=first_row,
            row_count=row_count,
            groups=groups,
            cores=cores,
            has_acc=acc is not None,
            splits=splits,
        )

    return pl.pallas_call(
        body,
        in_specs=specs,
        out_specs=out_specs,
        scratch_shapes=scratch,
        out_shape=out_shape,
        compiler_params=small(),
        cost_estimate=pl.CostEstimate(
            flops=2 * tokens * width * row_count,
            bytes_accessed=2 * width * row_count,
            transcendentals=0,
        ),
    )(*operands)


def join(pieces, column, width, after):
    rows = pieces[0].shape[0]

    def body(*refs):
        for n in range(len(pieces)):
            refs[-1][pl.ds(n * rows, rows), :] = refs[n][:, pl.ds(column, width)]

    return pl.pallas_call(
        body,
        in_specs=[VMEM] * len(pieces) + [ANY] * len(after),
        out_specs=VMEM,
        out_shape=jax.ShapeDtypeStruct((rows * len(pieces), width), pieces[0].dtype),
        compiler_params=small(),
    )(*pieces, *after)


def gate(grads, preacts, column):
    rows, width = grads.shape

    def body(grad_ref, preact_ref, out_ref):
        slope = silu_slope(preact_ref[:, pl.ds(column, width)].astype(jnp.float32))
        out_ref[...] = (slope * grad_ref[...].astype(jnp.float32)).astype(jnp.bfloat16)

    return pl.pallas_call(
        body,
        in_specs=[VMEM, VMEM],
        out_specs=VMEM,
        out_shape=jax.ShapeDtypeStruct((rows, width), jnp.bfloat16),
        compiler_params=small(),
    )(grads, preacts)


def combine(kept, arrived, residual, column, before):
    rows, width = kept.shape
    parts = len(arrived)

    def body(*refs):
        total = refs[0][...] + refs[1 + parts][:, pl.ds(column, width)].astype(jnp.float32)
        for ref in refs[1 : 1 + parts]:
            total = total + ref[...].astype(jnp.float32)
        value = total.astype(jnp.bfloat16)
        if before:
            outs = refs[2 + parts + len(before) :]
            for n in range(len(before)):
                outs[1][:, pl.ds(n * width, width)] = refs[2 + parts + n][...]
            outs[1][:, pl.ds(column, width)] = value
        else:
            outs = refs[2 + parts :]
        outs[0][...] = value

    out_shape = [jax.ShapeDtypeStruct((rows, width), jnp.bfloat16)]
    if before:
        out_shape.append(jax.ShapeDtypeStruct(residual.shape, jnp.bfloat16))
    operands = [kept, *arrived, residual, *before]
    return pl.pallas_call(
        body,
        in_specs=[VMEM] * len(operands),
        out_specs=[VMEM] * len(out_shape),
        out_shape=out_shape,
        compiler_params=small(),
    )(*operands)


def finish(parts, arrived, residual, earlier, terms):
    rows = residual.shape[0]
    width = parts[0].shape[1]
    count = len(parts)
    per_part = len(arrived[0])

    def body(*refs):
        layer = spot()[0]
        out_ref, score_ref = refs[-2:]
        term_refs = refs[-2 - len(terms) : -2]
        residual_ref = refs[count * (1 + per_part)]
        earlier_refs = refs[count * (1 + per_part) + 1 : -2 - len(terms)]
        for n in range(count):
            span = pl.ds(n * width, width)
            total = refs[n][...] + residual_ref[:, span].astype(jnp.float32)
            for d in range(per_part):
                total = total + refs[count + n * per_part + d][...].astype(jnp.float32)
            value = total.astype(jnp.bfloat16)
            for tick, ref in enumerate(earlier_refs):
                value = jnp.where(layer == LAYERS - 1 - tick, ref[:, span], value)
            out_ref[:, span] = value
        values = [ref[...] for ref in term_refs]
        while len(values) > 1:
            values = [values[n] + values[n + 1] for n in range(0, len(values), 2)]
        score_ref[...] = values[0]

    operands = [*parts]
    for group in arrived:
        operands += group
    operands += [residual, *earlier, *terms]
    return pl.pallas_call(
        body,
        in_specs=[VMEM] * len(operands),
        out_specs=[VMEM, VMEM],
        out_shape=[
            jax.ShapeDtypeStruct((rows, width * count), jnp.bfloat16),
            jax.ShapeDtypeStruct(terms[0].shape, terms[0].dtype),
        ],
        compiler_params=small(),
    )(*operands)


def left_side(values, factors):
    def body(value_ref, factor_ref, out_ref):
        out_ref[...] = jnp.dot(
            value_ref[...], factor_ref[...], preferred_element_type=jnp.float32
        )

    return pl.pallas_call(
        body,
        in_specs=[VMEM, VMEM],
        out_specs=VMEM,
        out_shape=jax.ShapeDtypeStruct((values.shape[0], factors.shape[1]), jnp.float32),
        compiler_params=small(),
    )(values, factors)


def score_terms(ids, preacts, candidates, factors, left, seqs):
    def body(id_ref, preact_ref, *refs):
        layer, _, _, _, group = spot()
        factor_ref, left_ref, out_ref = refs[-3:]
        value = refs[0][...]
        for tick, ref in enumerate(refs[1:-3]):
            value = jnp.where(layer == LAYERS - 2 - tick, ref[...], value)
        slope = silu_slope(preact_ref[...].astype(jnp.float32))
        gate = (slope * value.astype(jnp.float32)).astype(jnp.bfloat16)
        right = jnp.dot(gate, factor_ref[...], preferred_element_type=jnp.float32)
        terms = left_ref[...] * right
        rank = lax.broadcasted_iota(jnp.int32, (terms.shape[1], QUERIES), 0) // RANK
        query = lax.broadcasted_iota(jnp.int32, (terms.shape[1], QUERIES), 1)
        pick = (rank == query).astype(jnp.float32)
        tokens = terms.shape[0]
        slot = group * seqs + lax.broadcasted_iota(jnp.int32, (seqs, tokens), 0)
        member = (id_ref[...] == slot).astype(jnp.float32)
        total = jnp.dot(
            member, terms, preferred_element_type=jnp.float32, precision=lax.Precision.HIGHEST
        )
        out_ref[...] = jnp.dot(
            total, pick, preferred_element_type=jnp.float32, precision=lax.Precision.HIGHEST
        )

    operands = [ids, preacts, *candidates, factors, left]
    return pl.pallas_call(
        body,
        in_specs=[VMEM] * len(operands),
        out_specs=VMEM,
        out_shape=jax.ShapeDtypeStruct((seqs, QUERIES), jnp.float32),
        compiler_params=small(),
    )(*operands)


def per_device(
    cotangent, lengths, example_ids, layer_inputs, preacts, weights, query_left, query_right
):
    blocks = lax.axis_size("section") // LAYERS
    groups = lax.axis_size("dp")
    cores = blocks // groups
    tokens = cotangent.shape[0]
    width = layer_inputs.shape[1]
    part = width // CHUNKS
    seqs = lengths.shape[0]

    def device(s, h, k, y):
        return ((s * blocks) + h * cores + k) * groups + y

    everyone = [
        (s, h, k, y)
        for s in range(LAYERS)
        for h in range(groups)
        for k in range(cores)
        for y in range(groups)
    ]

    def send(value, target):
        pairs = []
        for spot in everyone:
            goal = target(*spot)
            if goal[0] >= 0:
                pairs.append((device(*spot), device(*goal)))
        return lax.ppermute(value, AXES, pairs)

    def turned(value):
        return send(value, lambda s, h, k, y: (s, y, k, h))

    def lowered(value, tick, turn):
        def target(s, h, k, y):
            if s != LAYERS - 1 - tick:
                return (-1, 0, 0, 0)
            return (s - 1, y, k, h) if turn else (s - 1, h, k, y)

        return send(value, target)

    def from_places(value):
        return [
            send(value, lambda s, h, k, y: (s, (h - d) % groups, k, y))
            for d in range(1, groups)
        ]

    def from_cores(value):
        return [
            send(value, lambda s, h, k, y: (s, h, (k - d) % cores, y)) for d in range(1, cores)
        ]

    def sum_over(value, axis, count):
        step = 1
        while step < count:
            if axis == "core":
                value = value + send(value, lambda s, h, k, y: (s, h, k ^ step, y))
            elif axis == "place":
                value = value + send(value, lambda s, h, k, y: (s, h ^ step, k, y))
            else:
                value = value + send(value, lambda s, h, k, y: (s ^ step, h, k, y))
            step *= 2
        return value

    id_row = example_ids.reshape(1, tokens)
    top_grad, payload = begin(lengths, id_row, preacts, cotangent)

    turned_payload = turned(payload)
    crossed = [
        send(payload, lambda s, h, k, y: (s, (y - d) % groups, k, h))
        for d in range(1, groups)
    ]
    held = [load(weights, o, cores) for o in range(CHUNKS)]
    left_sum = left_side(layer_inputs, query_left)
    residual = top_grad
    candidates = [top_grad]
    sums = []
    for tick in range(LAYERS):
        last = tick == LAYERS - 1
        acc = None
        parts = []
        if tick == 0:
            owned = [[turned_payload] + crossed] * CHUNKS
        else:
            owned = [[gates[o]] + from_places(gates[o]) for o in range(CHUNKS)]
        behind = []
        if tick == 1:
            left_sum = sum_over(left_sum, "core", cores)
            behind = [left_sum]
        if tick == 2:
            left_sum = sum_over(left_sum, "place", groups)
            behind = [left_sum]
        if last:
            terms = score_terms(id_row, preacts, candidates, query_right, left_sum, seqs)
            terms = sum_over(terms, "core", cores)
            terms = sum_over(terms, "place", groups)
        for o in range(CHUNKS):
            column = o * part if tick == 0 else 0
            behind_join = [acc] if tick and o else []
            mine = join(owned[o], column, part, behind_join)
            pieces = [mine] + from_cores(mine)
            for k in range(cores):
                if o == CHUNKS - 1 and k == cores - 1:
                    for n in range(CHUNKS):
                        parts.append(
                            product(
                                pieces[k], held[o], acc, tick, k, n * part, part, groups, cores,
                                True, behind + [p[0] for p in parts[:n]],
                            )
                        )
                else:
                    acc = product(pieces[k], held[o], acc, tick, k, 0, width, groups, cores, False)
        arrived = []
        for n in range(CHUNKS):
            arrived.append(
                [
                    send(parts[n][d], lambda s, h, k, y: (s, h, k, (y + d) % groups))
                    for d in range(1, groups)
                ]
            )
        kept = [piece[0] for piece in parts]
        if last:
            break
        in_parts = []
        for n in range(CHUNKS):
            outs = combine(
                kept[n], arrived[n], residual, n * part, in_parts if n == CHUNKS - 1 else []
            )
            in_parts.append(outs[0])
        in_grad = outs[1]
        sums.append(in_grad)
        gates = []
        for n in range(CHUNKS):
            came = lowered(in_parts[n], tick, True)
            gates.append(gate(came, turned_payload, n * part))
        residual = lowered(in_grad, tick, False)
        candidates.append(residual)

    everywhere = [terms]
    for d in range(1, LAYERS):
        everywhere.append(send(terms, lambda s, h, k, y: (s ^ d, h, k, y)))
    result, scores = finish(kept, arrived, residual, sums, everywhere)
    return (result, scores)


def solution(mesh):
    placed = (
        P("dp", None),
        P("dp"),
        P("dp"),
        P("dp", "section"),
        P("dp", "section"),
        P("section", "dp"),
        P("section", None),
        P("section", None),
    )
    return jax.shard_map(
        per_device,
        mesh=mesh,
        in_specs=placed,
        out_specs=(P("dp", "section"), P("dp", None)),
        check_vma=False,
    )
```
